32 devices in a mesh: vert: 8 (over z, y), col: 4 (over x, core).
Axes of the slice: x: 2, y: 2, z: 4, core: 2. Of those that a mesh axis runs over, the one named last changes fastest.
Arguments:
- coeffs: bfloat16 [64, 400], P(('vert', 'col')), may hold values from -6 to 6
- shape_basis: bfloat16 [400, 3, 656], P('col', None, 'vert'), may hold values from -0.3125 to 0.3125
- template: float32 [3, 656], P(None, 'vert'), may hold values from -6 to 6
- regressor: float32 [55, 656], P(None, 'vert'), may hold values from -0.5 to 0.5
- quaternions: float32 [64, 4, 55], P(('vert', 'col')), may hold values from -1.5 to 1.5, as said below
- translation: float32 [64, 3], P(('vert', 'col')), may hold values from -6 to 6
- parents: int32 [55], replicated, may hold values from 0 to 53, as said below
- skin_index: int32 [656, 4], P('vert'), may hold values from 0 to 54, all different within a row
- skin_raw: float32 [656, 4], P('vert'), may hold values from 0.1 to 1
Outputs:
- posed_vertices: bfloat16 [64, 3, 656], P(('vert', 'col'))
The draws below stay inside these ranges and needn't reach their ends.
Inputs may be any that keep to these rules, and one draw needn't show every extreme that they name: parents[0] = 0 and parents[j] < j for j >= 1. `skin_index`: the four joints of a vertex differ. `quaternions`: component 0 lies in [0.5, 1.5].
All inputs are finite; a program needn't handle non-finite values.
Results may differ from the reference program's by a relative error of at most 0.0024.
Values may be sent and summed in bfloat16 or wider, within the bound.
A program may use at most 64 MiB of HBM per device.

```python
import math
import jax
import jax.numpy as jnp
from jax import lax

K = 400
J = 55
V = 656
CHARS = 64
N_VERT = 8


def draw_quaternions(key, part):
    first_key = jax.random.fold_in(key, 11)
    second_key = jax.random.fold_in(key, 12)
    scalar_part = jax.random.uniform(first_key, (CHARS, 1, J), jnp.float32, 0.75, 1.25)
    vector_part = jnp.clip(0.4 * jax.random.normal(second_key, (CHARS, 3, J), jnp.float32), -1.5, 1.5)
    return jnp.concatenate([scalar_part, vector_part], axis=1)


def draw_parents(key, part):
    steps_back = jax.random.randint(jax.random.fold_in(key, 21), (J,), 0, 3)
    joint_ids = jnp.arange(J, dtype=jnp.int32)
    return jnp.maximum(joint_ids - 1 - steps_back, 0).astype(jnp.int32)


def level_of(own_key, shape, split, smallest, largest):
    factor_of = 1.0
    for dim, parts in split:
        draws = jax.random.uniform(jax.random.fold_in(jax.random.fold_in(own_key, 6), dim), (parts,), jnp.float32, smallest / len(split), largest / len(split))
        factor_of = factor_of * jnp.repeat(jnp.exp(draws), shape[dim] // parts).reshape((-1,) + (1,) * (len(shape) - 1 - dim))
    return factor_of


def picks_of(key, rows, count, top, lift):
    order = jax.random.permutation(jax.random.fold_in(key, 1), count)
    favour = order
    for power in range(3):
        favour = favour * favour // count
    favour = favour * lift // count
    tickets = jax.random.randint(jax.random.fold_in(key, 2), (rows, count), 0, 4096) + favour
    fixed_rows = jax.random.permutation(jax.random.fold_in(key, 3), rows)[jnp.arange(count) % rows]
    tickets = jnp.where(jnp.arange(rows)[:, None] == fixed_rows[None, :], 1 << 14, tickets)
    priority = tickets * count + jnp.arange(count)
    return lax.top_k(priority.astype(jnp.int32), top)[1].astype(jnp.int32)


def centred(own_key, shape, spread, bound, shards=(), kind=jnp.bfloat16):
    entries = spread * jax.random.normal(own_key, shape, jnp.float32)
    if shards:
        entries = entries * level_of(own_key, shape, shards, -0.22, 0.18)
    return jnp.clip(entries, -bound, bound).astype(kind)


def setup_inputs(seed: int = 0) -> dict:
    seeds = jax.random.split(jax.random.key(seed), 10)
    coeffs = centred(seeds[0], (CHARS, K), 1.0, 6.0, ((0, 32),))
    shape_basis = centred(seeds[1], (K, 3, V), K ** -0.5, 0.3125, ((0, 4), (2, 8)))
    template = centred(seeds[2], (3, V), 1.0, 6.0, ((1, 8),), jnp.float32)
    regressor = centred(seeds[3], (J, V), (V // 4) ** -0.5, 0.5, ((1, 8),), jnp.float32)
    quaternions = draw_quaternions(jax.random.fold_in(seeds[9], 71), 0)
    translation = centred(seeds[5], (CHARS, 3), 1.0, 6.0, ((0, 32),), jnp.float32)
    parents = draw_parents(jax.random.fold_in(seeds[9], 71), 0)
    skin_index = picks_of(seeds[7], V, J, 4, 595)
    skin_raw = jnp.clip(jnp.exp(math.log(1.0) - 2.3025851 * jax.random.uniform(seeds[8], (V, 4), jnp.float32) ** level_of(seeds[8], (V, 4), ((0, 8),), -0.2, 0.2)), 0.1, 1.0)
    return dict(coeffs=coeffs, shape_basis=shape_basis, template=template, regressor=regressor, quaternions=quaternions, translation=translation, parents=parents, skin_index=skin_index, skin_raw=skin_raw)


def rotations(quaternions):
    quat_w = jnp.transpose(quaternions[:, 0])
    quat_x = jnp.transpose(quaternions[:, 1])
    quat_y = jnp.transpose(quaternions[:, 2])
    quat_z = jnp.transpose(quaternions[:, 3])
    scale_two = 2.0 / (quat_w * quat_w + quat_x * quat_x + quat_y * quat_y + quat_z * quat_z)
    matrix_rows = [
        [1.0 - scale_two * (quat_y * quat_y + quat_z * quat_z), scale_two * (quat_x * quat_y - quat_w * quat_z), scale_two * (quat_x * quat_z + quat_w * quat_y)],
        [scale_two * (quat_x * quat_y + quat_w * quat_z), 1.0 - scale_two * (quat_x * quat_x + quat_z * quat_z), scale_two * (quat_y * quat_z - quat_w * quat_x)],
        [scale_two * (quat_x * quat_z - quat_w * quat_y), scale_two * (quat_y * quat_z + quat_w * quat_x), 1.0 - scale_two * (quat_x * quat_x + quat_y * quat_y)],
    ]
    return jnp.stack([jnp.stack(entry, axis=1) for entry in matrix_rows], axis=1)


def kinematics(joints, quaternions, translation, parents):
    joint_total = quaternions.shape[2]
    local_rots = rotations(quaternions)
    places = jnp.transpose(joints, (2, 1, 0))
    glob_rot = jnp.zeros_like(local_rots).at[0].set(local_rots[0])
    glob_pos = jnp.zeros_like(places).at[0].set(places[0] + jnp.transpose(translation))

    def compose(joint, state_pair):
        rot_now, pos_now = state_pair
        parent = lax.dynamic_index_in_dim(parents, joint, 0, keepdims=False)
        parent_rot = lax.dynamic_index_in_dim(rot_now, parent, 0, keepdims=False)
        parent_pos = lax.dynamic_index_in_dim(pos_now, parent, 0, keepdims=False)
        local_rot = lax.dynamic_index_in_dim(local_rots, joint, 0, keepdims=False)
        offset = lax.dynamic_index_in_dim(places, joint, 0, keepdims=False) - lax.dynamic_index_in_dim(places, parent, 0, keepdims=False)
        new_rot = jnp.einsum("amc,mbc->abc", parent_rot, local_rot, precision=lax.Precision.HIGHEST)
        new_pos = jnp.einsum("amc,mc->ac", parent_rot, offset, precision=lax.Precision.HIGHEST) + parent_pos
        rot_now = lax.dynamic_update_index_in_dim(rot_now, new_rot, joint, 0)
        pos_now = lax.dynamic_update_index_in_dim(pos_now, new_pos, joint, 0)
        return (rot_now, pos_now)

    glob_rot, glob_pos = lax.fori_loop(1, joint_total, compose, (glob_rot, glob_pos))
    correction = glob_pos - jnp.einsum("jamc,jmc->jac", glob_rot, places, precision=lax.Precision.HIGHEST)
    frames = jnp.concatenate([glob_rot.reshape(joint_total, 9, glob_rot.shape[3]), correction], axis=1)
    return jnp.transpose(frames, (2, 1, 0))


def dense_weights(joint_index, raw_weights, joint_total):
    shares = raw_weights / jnp.sum(raw_weights, axis=1, keepdims=True)
    matches = joint_index[None, :, :] == jnp.arange(joint_total, dtype=jnp.int32)[:, None, None]
    return jnp.sum(jnp.where(matches, shares[None, :, :], jnp.zeros_like(shares)[None, :, :]), axis=2)


def apply_frames(blended, shaped_wide):
    coords = []
    for axis_out in range(3):
        value = blended[:, 9 + axis_out]
        for axis_in in range(3):
            value = value + blended[:, 3 * axis_out + axis_in] * shaped_wide[:, axis_in]
        coords.append(value)
    return jnp.stack(coords, axis=1)


def reference(coeffs, shape_basis, template, regressor, quaternions, translation, parents, skin_index, skin_raw):
    components = shape_basis.shape[0]
    vert_total = shape_basis.shape[2]
    flat_basis = shape_basis.reshape(components, 3 * vert_total)
    base_row = template.reshape(1, 3 * vert_total)
    weight_grid = dense_weights(skin_index, skin_raw, J)
    basis_table = jnp.einsum("kmv,jv->kmj", shape_basis.astype(jnp.float32), regressor, precision=lax.Precision.HIGHEST)
    base_table = jnp.einsum("mv,jv->mj", template, regressor, precision=lax.Precision.HIGHEST)
    block_size = CHARS // N_VERT

    def block_pass(inputs):
        coeff_block, quat_block, shift_block = inputs
        shaped = (jnp.dot(coeff_block, flat_basis, preferred_element_type=jnp.float32) + base_row).astype(jnp.bfloat16)
        shaped_wide = shaped.reshape(block_size, 3, vert_total).astype(jnp.float32)
        joints = jnp.einsum("ck,kmj->cmj", coeff_block.astype(jnp.float32), basis_table, precision=lax.Precision.HIGHEST) + base_table[None]
        frames = kinematics(joints, quat_block, shift_block, parents)
        blended = jnp.einsum("cej,jv->cev", frames, weight_grid, precision=lax.Precision.HIGHEST)
        return apply_frames(blended, shaped_wide).astype(jnp.bfloat16)

    result = lax.map(block_pass, (coeffs.reshape(N_VERT, block_size, components), quaternions.reshape(N_VERT, block_size, 4, J), translation.reshape(N_VERT, block_size, 3)))
    return result.reshape(CHARS, 3, vert_total)
```

```python
import functools

import jax
import jax.numpy as jnp
from jax import lax
from jax.experimental import pallas as pl
from jax.experimental.pallas import tpu as pltpu
from jax.sharding import PartitionSpec as P

MESH = pl.DeviceIdType.MESH
LANES = 128
HALF = 64
SUB = 8
F32 = jnp.float32
BF16 = jnp.bfloat16
EXACT = lax.Precision.HIGHEST


def iota(shape, dim):
    return lax.broadcasted_iota(jnp.int32, shape, dim)


def dot(a, b, precision=None):
    return jnp.dot(a, b, precision=precision, preferred_element_type=F32)


def dot_nt(a, b, precision=None):
    return lax.dot_general(a, b, (((1,), (1,)), ((), ())), precision=precision, preferred_element_type=F32)


def each(count, step):
    if count <= 16:
        for k in range(1, count):
            step(k)
    else:

        def one(k, carry):
            step(k)
            return carry

        lax.fori_loop(1, count, one, 0)


def kernel(
    n_vert,
    n_col,
    parents_hbm,
    coeffs_hbm,
    basis_hbm,
    template_hbm,
    regressor_hbm,
    quat_hbm,
    shift_hbm,
    index_hbm,
    raw_hbm,
    out_ref,
    parents,
    coeff_in,
    bas,
    template,
    regressor,
    quat,
    shift,
    index_in,
    raw_in,
    quat_rows,
    coeff_rows,
    blocks,
    sent,
    got,
    tree,
    state,
    diff,
    locals_ref,
    weights,
    local_s,
    coeff_s,
    coeff_r,
    bas_s,
    bas_r,
    index_s,
    index_r,
    raw_s,
    raw_r,
    sent_s,
    sent_r,
):
    me = lax.axis_index("vert")
    col = lax.axis_index("col")
    own, _ = coeffs_hbm.shape
    _, block, comps = basis_hbm.shape
    joints = regressor_hbm.shape[0]
    rows = n_vert * SUB

    barrier = pltpu.get_barrier_semaphore()

    def vert_peer(k):
        return (lax.rem(me + k, n_vert), col)

    def col_peer(k):
        return (me, lax.rem(col + k, n_col))

    each(n_vert, lambda k: pl.semaphore_signal(barrier, inc=1, device_id=vert_peer(k), device_id_type=MESH))
    each(n_col, lambda k: pl.semaphore_signal(barrier, inc=1, device_id=col_peer(k), device_id_type=MESH))

    pairs = [
        (coeffs_hbm, coeff_in.at[me]),
        (basis_hbm, bas.at[col]),
        (index_hbm, index_in.at[me]),
        (raw_hbm, raw_in.at[me]),
        (parents_hbm, parents),
        (quat_hbm, quat),
        (shift_hbm, shift),
        (template_hbm, template),
        (regressor_hbm, regressor),
    ]
    loads = [pltpu.make_async_copy(src, dst, local_s.at[i]) for i, (src, dst) in enumerate(pairs)]
    for load in loads:
        load.start()

    sub8 = iota((SUB, LANES), 0)
    lane8 = iota((SUB, LANES), 1)
    axis_lane = jnp.minimum((lane8 % SUB) // own, 2)
    quat_rows[...] = jnp.zeros(quat_rows.shape, F32)
    weights[...] = jnp.zeros(weights.shape, F32)
    tree[...] = jnp.zeros(tree.shape, F32)
    state[...] = jnp.zeros(state.shape, F32)
    diff[...] = jnp.zeros(diff.shape, F32)
    sent[...] = jnp.zeros(sent.shape, F32)
    for load in loads:
        load.wait()

    def copies(src, dst, send, recv, peer_of):
        def make(k):
            return pltpu.make_async_remote_copy(
                src_ref=src, dst_ref=dst, send_sem=send.at[k], recv_sem=recv.at[k], device_id=peer_of(k), device_id_type=MESH
            )

        return make

    coeff_copy = copies(coeff_in.at[me], coeff_in.at[me], coeff_s, coeff_r, vert_peer)
    bas_copy = copies(bas.at[col], bas.at[col], bas_s, bas_r, col_peer)
    index_copy = copies(index_in.at[me], index_in.at[me], index_s, index_r, vert_peer)
    raw_copy = copies(raw_in.at[me], raw_in.at[me], raw_s, raw_r, vert_peer)

    pl.semaphore_wait(barrier, n_vert + n_col - 2)
    each(n_col, lambda k: bas_copy(k).start())
    lower = 1 - me // (n_vert // 2)
    each(n_vert, lambda k: coeff_copy(k + lower * (n_vert - 2 * k)).start())
    each(n_vert, lambda k: index_copy(k).start())
    each(n_vert, lambda k: raw_copy(k).start())

    for c in range(own):
        quat_rows[4 * c : 4 * c + 4, 0:joints] = quat[c]
    q_row = iota((LANES, SUB), 0)
    q_col = iota((LANES, SUB), 1)
    w, x, y, z = [
        jnp.transpose(dot((q_col == (q_row % own) * 4 + comp).astype(F32), quat_rows[...], EXACT))[0:HALF] for comp in range(4)
    ]
    s = 2.0 / (w * w + x * x + y * y + z * z)
    matrix = [
        [1.0 - s * (y * y + z * z), s * (x * y - w * z), s * (x * z + w * y)],
        [s * (x * y + w * z), 1.0 - s * (x * x + z * z), s * (y * z - w * x)],
        [s * (x * z - w * y), s * (y * z + w * x), 1.0 - s * (x * x + y * y)],
    ]
    for m in range(3):
        for b in range(3):
            locals_ref[m, pl.ds(b, HALF, stride=SUB), :] = matrix[m][b]

    def compose(j, above):
        at = pl.multiple_of(j * SUB, SUB)
        new = jnp.zeros((SUB, LANES), F32)
        for m in range(3):
            new = new + jnp.broadcast_to(above[m : m + 1, :], (SUB, LANES)) * locals_ref[m, pl.ds(at, SUB), :]
        mine = above + (lane8 % HALF == j).astype(F32)
        new = jnp.where(sub8 < 3, new, jnp.where(sub8 == 3, mine, 0.0))
        if isinstance(j, int):
            new = new + jnp.where((sub8 == 3) & (lane8 == joints), 1.0, 0.0)
        tree[j] = new
        state[pl.ds(at, SUB), :] = new
        diff[pl.ds(at, SUB), :] = above - new

    def descend(j, carry):
        compose(j, tree[parents[j]])
        return carry

    compose(0, (axis_lane == sub8).astype(F32))
    lax.fori_loop(1, joints, descend, 0)

    def flipped(ref, m, n):
        value = ref[pl.ds(m, HALF, stride=SUB), :]
        return jnp.transpose(jnp.concatenate([value, value], axis=0))[0:n]

    gains = [flipped(diff, m, SUB) for m in range(3)]
    gains = [jnp.where(lane8 < HALF, gain, 0.0) for gain in gains]
    factors = jnp.concatenate(
        [flipped(state, m, SUB)[:, 0:HALF] for m in range(3)] + [flipped(state, 3, HALF)[:, 0:HALF]], axis=0
    )
    moves = jnp.concatenate([shift[...]] * (SUB // own), axis=0)
    m_axis = jnp.minimum(iota(moves.shape, 0) // own, 2)
    moves = jnp.sum(jnp.where(iota(moves.shape, 1) == m_axis, moves, 0.0), axis=1, keepdims=True)
    moves = jnp.where(lane8 == joints, moves, 0.0)

    each(n_vert, lambda k: coeff_copy(k).wait_recv())
    for i in range(n_vert):
        one = coeff_in[i].astype(F32)
        coeff_rows[i * SUB : (i + 1) * SUB, 0 : n_col * comps] = jnp.concatenate([one] * (SUB // own), axis=0)
    for kb in range(n_col):
        blocks[kb] = coeff_rows[:, kb * comps : (kb + 1) * comps].astype(BF16)

    totals = [template[m : m + 1, :] + dot_nt(blocks[col], bas[col, m]) for m in range(3)]
    for k in range(1, n_col):
        bas_copy(k).wait_recv()
        source = lax.rem(col + n_col - k, n_col)
        totals = [totals[m] + dot_nt(blocks[source], bas[source, m]) for m in range(3)]
    r_axis = jnp.minimum((iota((rows, block), 0) % SUB) // own, 2)
    full = jnp.where(r_axis == 0, totals[0], jnp.where(r_axis == 1, totals[1], totals[2]))
    share = dot_nt(full, regressor[...], EXACT)
    sent[:, 0, :, 0:block] = full.astype(BF16).astype(F32).reshape(n_vert, SUB, block)
    sent[:, 1, :, 0:joints] = share.reshape(n_vert, SUB, joints)

    def sent_copy(k):
        target = lax.rem(me + k, n_vert)
        return pltpu.make_async_remote_copy(
            src_ref=sent.at[target],
            dst_ref=got.at[me],
            send_sem=sent_s.at[k],
            recv_sem=sent_r.at[k],
            device_id=(target, col),
            device_id_type=MESH,
        )

    each(n_vert, lambda k: sent_copy(k + lower * (n_vert - 2 * k)).start())
    got[me] = sent[me]

    each(n_vert, lambda k: index_copy(k).wait_recv())
    each(n_vert, lambda k: raw_copy(k).wait_recv())
    joint_row = iota((HALF, block), 0)
    for i in range(n_vert):
        raw = raw_in[i]
        raw = raw / jnp.sum(raw, axis=0, keepdims=True)
        index = index_in[i]
        grid = jnp.zeros((HALF, block), F32)
        for slot in range(raw.shape[0]):
            grid = jnp.where(index[slot : slot + 1, :] == joint_row, raw[slot : slot + 1, :], grid)
        weights[:, i * LANES : i * LANES + block] = grid
    blended = dot(factors, weights[...], EXACT)
    turns = [blended[m * SUB : (m + 1) * SUB] for m in range(3)]
    upper = blended[3 * SUB :]
    upper_hi = upper.astype(BF16)
    upper_lo = (upper - upper_hi.astype(F32)).astype(BF16)
    upper_all = jnp.concatenate([upper_hi, upper_lo, upper_hi], axis=0)

    def rows_of(tile):
        spun = [tile] + [pltpu.roll(tile, own * q, 0) for q in range(1, SUB // own)]
        count = SUB // own
        result = []
        for m in range(3):
            value = spun[(-m) % count]
            for q in range(1, count):
                value = jnp.where(sub8 // own == q, spun[(q - m) % count], value)
            result.append(value)
        return result

    each(n_vert, lambda k: sent_copy(k).wait_recv())
    summed = got[0, 1]
    for i in range(1, n_vert):
        summed = summed + got[i, 1]
    places = rows_of(summed)
    term = moves
    for m in range(3):
        term = term + gains[m] * places[m]
    term_hi = term.astype(BF16)
    term_lo = (term - term_hi.astype(F32)).astype(BF16)
    term_all = jnp.concatenate([term_hi[:, 0:HALF], term_hi[:, 0:HALF], term_lo[:, 0:HALF]], axis=1)
    moved = dot(term_all, upper_all)

    n_cols = -(-n_vert * block // LANES) + 1
    columns = [None] * n_cols

    def put(q, value):
        columns[q] = value if columns[q] is None else columns[q] + value

    for i in range(n_vert):
        q, r = divmod(i * block, LANES)
        at = slice(i * LANES, (i + 1) * LANES)
        shaped = rows_of(got[i, 0])
        tile = moved[:, at]
        for m in range(3):
            tile = tile + turns[m][:, at] * shaped[m]
        if r:
            tile = pltpu.roll(tile, r, 1)
        if r + block > LANES:
            put(q, jnp.where(lane8 >= r, tile, 0.0))
            put(q + 1, jnp.where(lane8 < r, tile, 0.0))
        else:
            put(q, tile)
    width = n_vert * block
    for q in range(n_cols):
        size = min(LANES, width - q * LANES)
        if size > 0:
            value = columns[q].astype(out_ref.dtype)
            for a in range(3):
                out_ref[a, :, q * LANES : q * LANES + size] = value[own * a : own * (a + 1), 0:size]

    each(n_vert, lambda k: coeff_copy(k).wait_send())
    each(n_col, lambda k: bas_copy(k).wait_send())
    each(n_vert, lambda k: index_copy(k).wait_send())
    each(n_vert, lambda k: raw_copy(k).wait_send())
    each(n_vert, lambda k: sent_copy(k).wait_send())


def body(n_vert, n_col, coeffs, shape_basis, template, regressor, quaternions, translation, parents, skin_index, skin_raw):
    own, total = coeffs.shape
    comps, _, block = shape_basis.shape
    joints = regressor.shape[0]
    slots = skin_index.shape[1]
    vmem = pl.BlockSpec(memory_space=pltpu.VMEM)
    anywhere = pl.BlockSpec(memory_space=pl.ANY)
    dma = pltpu.SemaphoreType.DMA
    out = pl.pallas_call(
        functools.partial(kernel, n_vert, n_col),
        out_shape=pltpu.VMEM((3, own, n_vert * block), BF16),
        in_specs=[anywhere] * 9,
        out_specs=vmem,
        scratch_shapes=[
            pltpu.SMEM((joints,), jnp.int32),
            pltpu.VMEM((n_vert, own, total), BF16),
            pltpu.VMEM((n_col, 3, block, comps), BF16),
            pltpu.VMEM((3, block), F32),
            pltpu.VMEM((joints, block), F32),
            pltpu.VMEM((own, 4, joints), F32),
            pltpu.VMEM((own, 3), F32),
            pltpu.VMEM((n_vert, slots, block), jnp.int32),
            pltpu.VMEM((n_vert, slots, block), F32),
            pltpu.VMEM((SUB, LANES), F32),
            pltpu.VMEM((n_vert * SUB, total), F32),
            pltpu.VMEM((n_col, n_vert * SUB, comps), BF16),
            pltpu.VMEM((n_vert, 2, SUB, LANES), F32),
            pltpu.VMEM((n_vert, 2, SUB, LANES), F32),
            pltpu.VMEM((joints, SUB, LANES), F32),
            pltpu.VMEM((HALF * SUB, LANES), F32),
            pltpu.VMEM((HALF * SUB, LANES), F32),
            pltpu.VMEM((3, HALF * SUB, LANES), F32),
            pltpu.VMEM((HALF, n_vert * LANES), F32),
            dma((9,)),
            dma((n_vert,)),
            dma((n_vert,)),
            dma((n_col,)),
            dma((n_col,)),
            dma((n_vert,)),
            dma((n_vert,)),
            dma((n_vert,)),
            dma((n_vert,)),
            dma((n_vert,)),
            dma((n_vert,)),
        ],
        compiler_params=pltpu.CompilerParams(collective_id=0, has_side_effects=True),
    )(
        parents,
        coeffs,
        jnp.transpose(shape_basis, (1, 2, 0)),
        template,
        regressor,
        quaternions,
        translation,
        jnp.transpose(skin_index),
        jnp.transpose(skin_raw),
    )
    return jnp.transpose(out, (1, 0, 2))


def solution(mesh):
    in_specs = (
        P(("vert", "col"), None),
        P("col", None, "vert"),
        P(None, "vert"),
        P(None, "vert"),
        P(("vert", "col"), None, None),
        P(("vert", "col"), None),
        P(),
        P("vert", None),
        P("vert", None),
    )
    out_specs = P(("vert", "col"), None, None)
    step = functools.partial(body, mesh.shape["vert"], mesh.shape["col"])
    return jax.shard_map(step, mesh=mesh, in_specs=in_specs, out_specs=out_specs, check_vma=False)
```

```python
import functools

import jax
import jax.numpy as jnp
from jax import lax
from jax.experimental import pallas as pl
from jax.experimental.pallas import tpu as pltpu
from jax.sharding import PartitionSpec as P

MESH = pl.DeviceIdType.MESH
LANES = 128
HALF = 64
SUB = 8
PARTS = 3
F32 = jnp.float32
BF16 = jnp.bfloat16
EXACT = lax.Precision.HIGHEST


def iota(shape, dim):
    return lax.broadcasted_iota(jnp.int32, shape, dim)


def dot(a, b, precision=None):
    return jnp.dot(a, b, precision=precision, preferred_element_type=F32)


def dot_nt(a, b, precision=None):
    return lax.dot_general(a, b, (((1,), (1,)), ((), ())), precision=precision, preferred_element_type=F32)


def each(first, count, step):
    if count - first <= 16:
        for k in range(first, count):
            step(k)
    else:

        def one(k, carry):
            step(k)
            return carry

        lax.fori_loop(first, count, one, 0)


def split(value):
    parts = []
    for _ in range(PARTS):
        part = value.astype(BF16)
        value = value - part.astype(F32)
        parts.append(part)
    return parts


def kernel(
    n_vert,
    n_col,
    parents_hbm,
    coeffs_hbm,
    basis_hbm,
    template_hbm,
    regressor_hbm,
    quat_hbm,
    shift_hbm,
    index_hbm,
    raw_hbm,
    out_ref,
    parents,
    coeff_in,
    bas,
    template,
    regressor,
    quat,
    shift,
    index_in,
    raw_in,
    quat_rows,
    coeff_out,
    coeff_got,
    passed,
    coeff_rows,
    skin_out,
    skin_got,
    spread,
    wide,
    table,
    bias,
    product,
    lead,
    sent,
    got,
    tree,
    state,
    diff,
    locals_ref,
    weights,
    local_s,
    bas_s,
    bas_r,
    coeff_s,
    coeff_r,
    passed_s,
    passed_r,
    relay_s,
    skin_s,
    skin_r,
    sent_s,
    sent_r,
):
    me = lax.axis_index("vert")
    col = lax.axis_index("col")
    own, total = coeffs_hbm.shape
    _, block, comps = basis_hbm.shape
    joints = regressor_hbm.shape[0]
    slots = index_hbm.shape[0]
    groups = n_col // 2
    n_src = n_vert * groups
    room = LANES - block
    extra = joints - room

    group = col // 2
    side = col % 2
    mine = me * groups + group
    first = mine == 0
    hub = n_vert // 2
    is_hub = (me == hub) & (col == 1)
    partner = (me, 2 * group + 1 - side)
    upper = me // hub

    def place(i, parity):
        return (i // groups, 2 * (i % groups) + parity)

    def across(i):
        return place(i, 1 - side)

    def far_first(j):
        return j + (1 - upper) * (n_src - 1 - 2 * j)

    barrier = pltpu.get_barrier_semaphore()

    def hello(target):
        pl.semaphore_signal(barrier, inc=1, device_id=target, device_id_type=MESH)

    @pl.when(is_hub)
    def _():
        hello((0, 1))

    @pl.when(is_hub | first)
    def _():
        hello(across(0))

    @pl.when((side == 1) & jnp.logical_not(is_hub))
    def _():
        hello((hub, 1))

    each(1, n_src, lambda j: hello(across(n_src - j)))

    pairs = [
        (coeffs_hbm, coeff_in),
        (basis_hbm, bas.at[side]),
        (index_hbm, index_in),
        (raw_hbm, raw_in),
        (parents_hbm, parents),
        (quat_hbm, quat),
        (shift_hbm, shift),
        (template_hbm, template),
        (regressor_hbm, regressor),
    ]
    loads = [pltpu.make_async_copy(src, dst, local_s.at[i]) for i, (src, dst) in enumerate(pairs)]
    for load in loads:
        load.start()

    sub8 = iota((SUB, LANES), 0)
    lane8 = iota((SUB, LANES), 1)
    axis_lane = jnp.minimum((lane8 % SUB) // own, 2)
    quat_rows[...] = jnp.zeros(quat_rows.shape, F32)
    weights[...] = jnp.zeros(weights.shape, F32)
    tree[...] = jnp.zeros(tree.shape, F32)
    state[...] = jnp.zeros(state.shape, F32)
    diff[...] = jnp.zeros(diff.shape, F32)
    coeff_out[...] = jnp.zeros(coeff_out.shape, BF16)
    spread[...] = jnp.zeros(spread.shape, F32)
    wide[...] = jnp.zeros(wide.shape, F32)
    bias[...] = jnp.zeros(bias.shape, F32)
    for load in loads:
        load.wait()

    mine_coeffs = coeff_in[...].astype(F32)
    for kb in range(n_col):
        coeff_out[kb, :, 0:comps] = mine_coeffs[:, kb * comps : (kb + 1) * comps].astype(BF16)
    raw = raw_in[...]
    skin_out[0] = index_in[...].astype(F32)
    skin_out[1] = raw / jnp.sum(raw, axis=0, keepdims=True)

    def remote(src, dst, send, recv, target):
        return pltpu.make_async_remote_copy(
            src_ref=src, dst_ref=dst, send_sem=send, recv_sem=recv, device_id=target, device_id_type=MESH
        )

    bas_copy = remote(bas.at[side], bas.at[side], bas_s, bas_r, partner)

    def bas_arrival():
        remote(bas.at[1 - side], bas.at[1 - side], bas_s, bas_r, partner).wait_recv()

    def two(i):
        return pl.ds(2 * (i % groups), 2)

    def coeff_copy(i):
        return remote(coeff_out.at[two(i)], coeff_got.at[mine], coeff_s.at[i], coeff_r.at[mine], across(i))

    def coeff_arrival(i):
        remote(coeff_out.at[pl.ds(0, 2)], coeff_got.at[i], coeff_s.at[i], coeff_r.at[i], across(i)).wait_recv()

    pass_copy = remote(coeff_out, passed.at[side], passed_s, passed_r.at[side], (hub, 1))

    def pass_arrival(k):
        remote(coeff_out, passed.at[k], passed_s, passed_r.at[k], (0, k)).wait_recv()

    def relay_copy(k, i):
        return remote(passed.at[k, two(i)], coeff_got.at[0], relay_s.at[k, i], coeff_r.at[0], place(i, 1 - k))

    def skin_copy(i):
        return remote(skin_out, skin_got.at[me], skin_s.at[i], skin_r.at[me], across(i))

    def skin_arrival(v):
        remote(skin_out, skin_got.at[v], skin_s.at[0], skin_r.at[v], partner).wait_recv()

    def tile(ref, i):
        start = i * SUB if isinstance(i, int) else pl.multiple_of(i * SUB, SUB)
        return ref.at[pl.ds(start, SUB)]

    def sent_copy(i):
        return remote(tile(sent, i), tile(got, mine), sent_s.at[i], sent_r.at[mine], across(i))

    lead_copy = remote(lead, tile(got, mine), sent_s.at[0], sent_r.at[mine], across(0))

    def sent_arrival(i):
        remote(tile(sent, i), tile(got, i), sent_s.at[i], sent_r.at[i], across(i)).wait_recv()

    hub_index = hub * groups
    expected = n_src + is_hub.astype(jnp.int32) * (n_src - 1)
    pl.semaphore_wait(barrier, jnp.where(first, 2, expected))
    bas_copy.start()

    @pl.when(first)
    def _():
        pass_copy.start()

    @pl.when(jnp.logical_not(first))
    def _():
        each(0, n_src, lambda j: coeff_copy(far_first(j)).start())

    @pl.when(is_hub)
    def _():
        pass_arrival(0)
        each(hub_index + 1, n_src, lambda i: relay_copy(0, i).start())
        pltpu.make_async_copy(passed.at[0, two(hub_index)], coeff_got.at[0], coeff_r.at[0]).start()
        each(0, hub_index, lambda i: relay_copy(0, i).start())
        pass_arrival(1)
        each(0, n_src, lambda j: relay_copy(1, n_src - 1 - j).start())

    @pl.when(group == groups - 1)
    def _():
        each(0, n_src, lambda j: skin_copy(far_first(j)).start())

    for c in range(own):
        quat_rows[4 * c : 4 * c + 4, 0:joints] = quat[c]
    q_row = iota((LANES, SUB), 0)
    q_col = iota((LANES, SUB), 1)
    w, x, y, z = [
        jnp.transpose(dot((q_col == (q_row % own) * 4 + comp).astype(F32), quat_rows[...], EXACT))[0:HALF] for comp in range(4)
    ]
    s = 2.0 / (w * w + x * x + y * y + z * z)
    matrix = [
        [1.0 - s * (y * y + z * z), s * (x * y - w * z), s * (x * z + w * y)],
        [s * (x * y + w * z), 1.0 - s * (x * x + z * z), s * (y * z - w * x)],
        [s * (x * z - w * y), s * (y * z + w * x), 1.0 - s * (x * x + y * y)],
    ]
    for m in range(3):
        for b in range(3):
            locals_ref[m, pl.ds(b, HALF, stride=SUB), :] = matrix[m][b]

    def compose(j, above):
        at = pl.multiple_of(j * SUB, SUB)
        new = jnp.zeros((SUB, LANES), F32)
        for m in range(3):
            new = new + jnp.broadcast_to(above[m : m + 1, :], (SUB, LANES)) * locals_ref[m, pl.ds(at, SUB), :]
        mine = above + (lane8 % HALF == j).astype(F32)
        new = jnp.where(sub8 < 3, new, jnp.where(sub8 == 3, mine, 0.0))
        if isinstance(j, int):
            new = new + jnp.where((sub8 == 3) & (lane8 == joints), 1.0, 0.0)
        tree[j] = new
        state[pl.ds(at, SUB), :] = new
        diff[pl.ds(at, SUB), :] = above - new

    def descend(j, carry):
        compose(j, tree[parents[j]])
        return carry

    compose(0, (axis_lane == sub8).astype(F32))
    lax.fori_loop(1, joints, descend, 0)

    for m in range(3):
        spread[m, block:LANES, :] = regressor[0:room, :]
        spread[m, extra * m : extra * (m + 1), :] = regressor[room:joints, :]
    for m in range(3):
        base = dot_nt(template[...], spread[m], EXACT)[m : m + 1, :]
        spot = iota(base.shape, 1)
        bias[m : m + 1, :] = jnp.where(spot >= block, base, 0.0)
        bias[m : m + 1, 0:block] = template[m : m + 1, :]
        mark = (spot >= extra * m) & (spot < extra * (m + 1))
        bias[3:4, :] = bias[3:4, :] + jnp.where(mark, base, 0.0)
    spread_parts = [jnp.concatenate(split(spread[m]), axis=0) for m in range(3)]

    def lay(b, at):
        for m in range(3):
            one = bas[b, m]
            sums = dot(spread_parts[m], one)
            sums = sums[0:LANES] + sums[LANES : 2 * LANES] + sums[2 * LANES :]
            wide[m * LANES : m * LANES + block, at : at + comps] = one.astype(F32)
            wide[m * LANES + block : (m + 1) * LANES, at : at + comps] = sums[block:]
            row = 3 * LANES + extra * m
            wide[row : row + extra, at : at + comps] = sums[extra * m : extra * (m + 1)]

    bas_arrival()
    for b in range(2):
        lay(b, b * LANES)
    for p, part in enumerate(split(wide[...])):
        table[p] = part

    has_bias = (group == 0).astype(F32)

    def partial(rows, q):
        at = slice(q * LANES, (q + 1) * LANES)
        value = bias[q : q + 1, :] * has_bias
        for p in range(PARTS):
            value = value + dot_nt(rows, table[p, at, :])
        return value

    coeff_arrival(0)
    rows = jnp.concatenate([coeff_got[0, 0], coeff_got[0, 1]], axis=1)
    lead[...] = jnp.concatenate([partial(rows, q) for q in range(4)], axis=0)
    lead_copy.start()

    each(1, n_src, coeff_arrival)
    per = SUB // own

    def gather(step):
        for b in range(2):
            rows = [coeff_got[step * per + i, b].astype(F32) for i in range(per)]
            start = step * SUB if isinstance(step, int) else pl.multiple_of(step * SUB, SUB)
            coeff_rows[pl.ds(start, SUB), b * LANES : (b + 1) * LANES] = jnp.concatenate(rows, axis=0)

    each(0, n_src // per, gather)
    rows = coeff_rows[...].astype(BF16)
    for q in range(4):
        product[q] = partial(rows, q)
    for q in range(4):
        for c in range(own):
            value = product[q, pl.ds(c, n_src, stride=own), :]
            sent[pl.ds(q * own + c, n_src, stride=SUB), :] = value
    each(0, n_src - 1, lambda j: sent_copy(1 + j + (1 - upper) * (n_src - 2 - 2 * j)).start())

    def flipped(ref, m, n):
        value = ref[pl.ds(m, HALF, stride=SUB), :]
        return jnp.transpose(jnp.concatenate([value, value], axis=0))[0:n]

    gains = [flipped(diff, m, SUB) for m in range(3)]
    gains = [jnp.where(lane8 < HALF, gain, 0.0) for gain in gains]
    factors = jnp.concatenate(
        [flipped(state, m, SUB)[:, 0:HALF] for m in range(3)] + [flipped(state, 3, HALF)[:, 0:HALF]], axis=0
    )
    moves = jnp.concatenate([shift[...]] * (SUB // own), axis=0)
    m_axis = jnp.minimum(iota(moves.shape, 0) // own, 2)
    moves = jnp.sum(jnp.where(iota(moves.shape, 1) == m_axis, moves, 0.0), axis=1, keepdims=True)
    moves = jnp.where(lane8 == joints, moves, 0.0)

    each(0, n_vert, skin_arrival)
    joint_row = iota((HALF, block), 0).astype(F32)
    for i in range(n_vert):
        grid = jnp.zeros((HALF, block), F32)
        for slot in range(slots):
            grid = jnp.where(skin_got[i, 0, slot : slot + 1, :] == joint_row, skin_got[i, 1, slot : slot + 1, :], grid)
        weights[:, i * LANES : i * LANES + block] = grid
    blended = dot(factors, weights[...], EXACT)
    turns = [blended[m * SUB : (m + 1) * SUB] for m in range(3)]
    above_hi = blended[3 * SUB :].astype(BF16)
    above_lo = (blended[3 * SUB :] - above_hi.astype(F32)).astype(BF16)
    above_all = jnp.concatenate([above_hi, above_lo, above_hi], axis=0)

    def rows_of(value):
        count = SUB // own
        spun = [value] + [pltpu.roll(value, own * q, 0) for q in range(1, count)]
        result = []
        for m in range(3):
            one = spun[(-m) % count]
            for q in range(1, count):
                one = jnp.where(sub8 // own == q, spun[(q - m) % count], one)
            result.append(one)
        return result

    each(0, n_src, sent_arrival)
    tiles = []
    for i in range(n_vert):
        at = i * groups * SUB
        value = got[at : at + SUB, :]
        for q in range(1, groups):
            value = value + got[at + q * SUB : at + (q + 1) * SUB, :]
        tiles.append(value)
    summed = tiles[0]
    for value in tiles[1:]:
        summed = summed + value
    spots = jnp.where(lane8 < room, pltpu.roll(summed, room, 1), 0.0)
    for m in range(3):
        moved = pltpu.roll(pltpu.roll(summed, (room - extra * m) % LANES, 1), (own * (m - 3)) % SUB, 0)
        spots = jnp.where((sub8 // own == m) & (lane8 >= room) & (lane8 < joints), moved, spots)
    places = rows_of(spots)
    term = moves
    for m in range(3):
        term = term + gains[m] * places[m]
    term_hi = term.astype(BF16)
    term_lo = (term - term_hi.astype(F32)).astype(BF16)
    term_all = jnp.concatenate([term_hi[:, 0:HALF], term_hi[:, 0:HALF], term_lo[:, 0:HALF]], axis=1)
    moved = dot(term_all, above_all)

    n_cols = -(-n_vert * block // LANES) + 1
    columns = [None] * n_cols

    def put(q, value):
        columns[q] = value if columns[q] is None else columns[q] + value

    for i in range(n_vert):
        q, r = divmod(i * block, LANES)
        at = slice(i * LANES, (i + 1) * LANES)
        shaped = rows_of(tiles[i].astype(BF16).astype(F32))
        value = moved[:, at]
        for m in range(3):
            value = value + turns[m][:, at] * shaped[m]
        if r:
            value = pltpu.roll(value, r, 1)
        if r + block > LANES:
            put(q, jnp.where(lane8 >= r, value, 0.0))
            put(q + 1, jnp.where(lane8 < r, value, 0.0))
        else:
            put(q, value)
    width = n_vert * block
    for q in range(n_cols):
        size = min(LANES, width - q * LANES)
        if size > 0:
            value = columns[q].astype(out_ref.dtype)
            for a in range(3):
                out_ref[a, :, q * LANES : q * LANES + size] = value[own * a : own * (a + 1), 0:size]

    bas_copy.wait_send()

    @pl.when(first)
    def _():
        pass_copy.wait_send()

    @pl.when(jnp.logical_not(first))
    def _():
        each(0, n_src, lambda i: coeff_copy(i).wait_send())

    @pl.when(is_hub)
    def _():
        each(0, hub_index, lambda i: relay_copy(0, i).wait_send())
        each(hub_index + 1, n_src, lambda i: relay_copy(0, i).wait_send())
        each(0, n_src, lambda i: relay_copy(1, i).wait_send())

    @pl.when(group == groups - 1)
    def _():
        each(0, n_src, lambda i: skin_copy(i).wait_send())

    lead_copy.wait_send()
    each(1, n_src, lambda i: sent_copy(i).wait_send())


def body(n_vert, n_col, coeffs, shape_basis, template, regressor, quaternions, translation, parents, skin_index, skin_raw):
    own, total = coeffs.shape
    comps, _, block = shape_basis.shape
    joints = regressor.shape[0]
    slots = skin_index.shape[1]
    n_src = n_vert * (n_col // 2)
    anywhere = pl.BlockSpec(memory_space=pl.ANY)
    dma = pltpu.SemaphoreType.DMA
    out = pl.pallas_call(
        functools.partial(kernel, n_vert, n_col),
        out_shape=pltpu.VMEM((3, own, n_vert * block), BF16),
        in_specs=[anywhere] * 9,
        out_specs=pl.BlockSpec(memory_space=pltpu.VMEM),
        scratch_shapes=[
            pltpu.SMEM((joints,), jnp.int32),
            pltpu.VMEM((own, total), BF16),
            pltpu.VMEM((2, 3, block, comps), BF16),
            pltpu.VMEM((3, block), F32),
            pltpu.VMEM((joints, block), F32),
            pltpu.VMEM((own, 4, joints), F32),
            pltpu.VMEM((own, 3), F32),
            pltpu.VMEM((slots, block), jnp.int32),
            pltpu.VMEM((slots, block), F32),
            pltpu.VMEM((SUB, LANES), F32),
            pltpu.VMEM((n_col, own, LANES), BF16),
            pltpu.VMEM((n_src, 2, own, LANES), BF16),
            pltpu.VMEM((2, n_col, own, LANES), BF16),
            pltpu.VMEM((n_src * own, 2 * LANES), F32),
            pltpu.VMEM((2, slots, block), F32),
            pltpu.VMEM((n_vert, 2, slots, block), F32),
            pltpu.VMEM((3, LANES, block), F32),
            pltpu.VMEM((4 * LANES, 2 * LANES), F32),
            pltpu.VMEM((PARTS, 4 * LANES, 2 * LANES), BF16),
            pltpu.VMEM((4, LANES), F32),
            pltpu.VMEM((4, n_src * own, LANES), F32),
            pltpu.VMEM((SUB, LANES), F32),
            pltpu.VMEM((n_src * SUB, LANES), F32),
            pltpu.VMEM((n_src * SUB, LANES), F32),
            pltpu.VMEM((joints, SUB, LANES), F32),
            pltpu.VMEM((HALF * SUB, LANES), F32),
            pltpu.VMEM((HALF * SUB, LANES), F32),
            pltpu.VMEM((3, HALF * SUB, LANES), F32),
            pltpu.VMEM((HALF, n_vert * LANES), F32),
            dma((9,)),
            dma,
            dma,
            dma((n_src,)),
            dma((n_src,)),
            dma,
            dma((2,)),
            dma((2, n_src)),
            dma((n_src,)),
            dma((n_vert,)),
            dma((n_src,)),
            dma((n_src,)),
        ],
        compiler_params=pltpu.CompilerParams(collective_id=0, has_side_effects=True),
    )(
        parents,
        coeffs,
        jnp.transpose(shape_basis, (1, 2, 0)),
        template,
        regressor,
        quaternions,
        translation,
        jnp.transpose(skin_index),
        jnp.transpose(skin_raw),
    )
    return jnp.transpose(out, (1, 0, 2))


def solution(mesh):
    in_specs = (
        P(("vert", "col"), None),
        P("col", None, "vert"),
        P(None, "vert"),
        P(None, "vert"),
        P(("vert", "col"), None, None),
        P(("vert", "col"), None),
        P(),
        P("vert", None),
        P("vert", None),
    )
    out_specs = P(("vert", "col"), None, None)
    step = functools.partial(body, mesh.shape["vert"], mesh.shape["col"])
    return jax.shard_map(step, mesh=mesh, in_specs=in_specs, out_specs=out_specs, check_vma=False)
```

```python
import functools

import jax
import jax.numpy as jnp
from jax import lax
from jax.experimental import pallas as pl
from jax.experimental.pallas import tpu as pltpu
from jax.sharding import PartitionSpec as P

MESH = pl.DeviceIdType.MESH
LANES = 128
HALF = 64
SUB = 8
PARTS = 2
F32 = jnp.float32
BF16 = jnp.bfloat16
EXACT = lax.Precision.HIGHEST


def iota(shape, dim):
    return lax.broadcasted_iota(jnp.int32, shape, dim)


def dot(a, b, precision=None):
    return jnp.dot(a, b, precision=precision, preferred_element_type=F32)


def dot_nt(a, b, precision=None):
    return lax.dot_general(a, b, (((1,), (1,)), ((), ())), precision=precision, preferred_element_type=F32)


def each(first, count, step):
    if count - first <= 16:
        for k in range(first, count):
            step(k)
    else:

        def one(k, carry):
            step(k)
            return carry

        lax.fori_loop(first, count, one, 0)


def split(value, count):
    parts = []
    for _ in range(count):
        part = value.astype(BF16)
        value = value - part.astype(F32)
        parts.append(part)
    return parts


def kernel(
    n_vert,
    n_col,
    parents_hbm,
    coeffs_hbm,
    basis_hbm,
    template_hbm,
    regressor_hbm,
    quat_hbm,
    shift_hbm,
    index_hbm,
    raw_hbm,
    out_ref,
    parents,
    coeff_in,
    bas,
    template,
    regressor,
    quat,
    shift,
    index_in,
    raw_in,
    quat_rows,
    coeff_out,
    coeff_got,
    passed,
    coeff_rows,
    skin_out,
    skin_got,
    spread,
    wide,
    table,
    bias,
    product,
    lead,
    sent,
    got,
    tree,
    state,
    diff,
    locals_ref,
    weights,
    local_s,
    bas_s,
    bas_r,
    coeff_s,
    coeff_r,
    lead_r,
    passed_s,
    passed_r,
    relay_s,
    skin_s,
    skin_r,
    sent_s,
    sent_r,
):
    me = lax.axis_index("vert")
    col = lax.axis_index("col")
    own, total = coeffs_hbm.shape
    _, block, comps = basis_hbm.shape
    joints = regressor_hbm.shape[0]
    slots = index_hbm.shape[0]
    groups = n_col // 2
    n_src = n_vert * groups
    room = LANES - block
    extra = joints - room

    group = col // 2
    side = col % 2
    mine = me * groups + group
    first = mine == 0
    hub = n_vert // 2
    is_hub = (me == hub) & (col == 1)
    partner = (me, 2 * group + 1 - side)
    upper = me // hub

    def place(i, parity):
        return (i // groups, 2 * (i % groups) + parity)

    def across(i):
        return place(i, 1 - side)

    def far_first(j):
        return j + (1 - upper) * (n_src - 1 - 2 * j)

    barrier = pltpu.get_barrier_semaphore()

    def hello(target):
        pl.semaphore_signal(barrier, inc=1, device_id=target, device_id_type=MESH)

    @pl.when(is_hub)
    def _():
        hello((0, 1))

    @pl.when(is_hub | first)
    def _():
        hello(across(0))

    @pl.when((side == 1) & jnp.logical_not(is_hub))
    def _():
        hello((hub, 1))

    each(1, n_src, lambda j: hello(across(j)))

    pairs = [
        (coeffs_hbm, coeff_in),
        (basis_hbm, bas.at[side]),
        (index_hbm, index_in),
        (raw_hbm, raw_in),
        (parents_hbm, parents),
        (quat_hbm, quat),
        (shift_hbm, shift),
        (template_hbm, template),
        (regressor_hbm, regressor),
    ]
    loads = [pltpu.make_async_copy(src, dst, local_s.at[i]) for i, (src, dst) in enumerate(pairs)]
    for load in loads:
        load.start()

    sub8 = iota((SUB, LANES), 0)
    lane8 = iota((SUB, LANES), 1)
    axis_lane = jnp.minimum((lane8 % SUB) // own, 2)
    quat_rows[...] = jnp.zeros(quat_rows.shape, F32)
    weights[...] = jnp.zeros(weights.shape, F32)
    tree[...] = jnp.zeros(tree.shape, F32)
    state[...] = jnp.zeros(state.shape, F32)
    diff[...] = jnp.zeros(diff.shape, F32)
    coeff_out[...] = jnp.zeros(coeff_out.shape, BF16)
    spread[...] = jnp.zeros(spread.shape, F32)
    wide[...] = jnp.zeros(wide.shape, F32)
    bias[...] = jnp.zeros(bias.shape, F32)
    for load in loads:
        load.wait()

    mine_coeffs = coeff_in[...].astype(F32)
    for kb in range(n_col):
        coeff_out[kb, :, 0:comps] = mine_coeffs[:, kb * comps : (kb + 1) * comps].astype(BF16)
    raw = raw_in[...]
    skin_out[0] = index_in[...].astype(F32)
    skin_out[1] = raw / jnp.sum(raw, axis=0, keepdims=True)

    def remote(src, dst, send, recv, target):
        return pltpu.make_async_remote_copy(
            src_ref=src, dst_ref=dst, send_sem=send, recv_sem=recv, device_id=target, device_id_type=MESH
        )

    bas_copy = remote(bas.at[side], bas.at[side], bas_s, bas_r, partner)

    def two(i):
        return pl.ds(2 * (i % groups), 2)

    half = n_src // 2

    def coeff_sem(i):
        return coeff_r.at[i // half]

    def coeff_copy(i):
        return remote(coeff_out.at[two(i)], coeff_got.at[mine], coeff_s, coeff_sem(mine), across(i))

    def arrival(ref, recv):
        remote(ref, ref, bas_s, recv, partner).wait_recv()

    def departure(ref, send):
        remote(ref, ref, send, bas_r, partner).wait_send()

    pass_copy = remote(coeff_out, passed.at[side], passed_s, passed_r.at[side], (hub, 1))

    def relay_copy(k, i):
        return remote(passed.at[k, two(i)], coeff_got.at[0], relay_s.at[k], lead_r, place(i, 1 - k))

    def skin_copy(i):
        return remote(skin_out, skin_got.at[me], skin_s.at[i // n_vert], skin_r, across(i))

    def tile(ref, i):
        start = i * SUB if isinstance(i, int) else pl.multiple_of(i * SUB, SUB)
        return ref.at[pl.ds(start, SUB)]

    def sent_copy(i):
        return remote(tile(sent.at[i // half], i % half), tile(got, mine), sent_s, sent_r, across(i))

    lead_copy = remote(lead, tile(got, mine), sent_s, sent_r, across(0))

    hub_index = hub * groups
    expected = n_src + is_hub.astype(jnp.int32) * (n_src - 1)
    pl.semaphore_wait(barrier, jnp.where(first, 2, expected))
    bas_copy.start()

    @pl.when(first)
    def _():
        pass_copy.start()

    @pl.when(is_hub)
    def _():
        arrival(passed.at[0], passed_r.at[0])
        each(0, half // 2, lambda j: relay_copy(0, n_src - 1 - j).start())
        arrival(passed.at[1], passed_r.at[1])
        each(0, half // 2, lambda j: relay_copy(1, n_src - 1 - j).start())
        each(half // 2, n_src - 1 - hub_index, lambda j: relay_copy(0, n_src - 1 - j).start())
        pltpu.make_async_copy(passed.at[0, two(hub_index)], coeff_got.at[0], lead_r).start()
        each(half // 2, n_src, lambda j: relay_copy(1, n_src - 1 - j).start())
        each(0, hub_index, lambda i: relay_copy(0, i).start())

    @pl.when(jnp.logical_not(first))
    def _():
        each(0, n_src, lambda j: coeff_copy(far_first(j)).start())

    for c in range(own):
        quat_rows[4 * c : 4 * c + 4, 0:joints] = quat[c]
    q_row = iota((LANES, SUB), 0)
    q_col = iota((LANES, SUB), 1)
    w, x, y, z = [
        jnp.transpose(dot((q_col == (q_row % own) * 4 + comp).astype(F32), quat_rows[...], EXACT))[0:HALF] for comp in range(4)
    ]
    s = 2.0 / (w * w + x * x + y * y + z * z)
    matrix = [
        [1.0 - s * (y * y + z * z), s * (x * y - w * z), s * (x * z + w * y)],
        [s * (x * y + w * z), 1.0 - s * (x * x + z * z), s * (y * z - w * x)],
        [s * (x * z - w * y), s * (y * z + w * x), 1.0 - s * (x * x + y * y)],
    ]
    for m in range(3):
        for b in range(3):
            locals_ref[m, pl.ds(b, HALF, stride=SUB), :] = matrix[m][b]

    def compose(j, above):
        at = pl.multiple_of(j * SUB, SUB)
        new = jnp.zeros((SUB, LANES), F32)
        for m in range(3):
            new = new + jnp.broadcast_to(above[m : m + 1, :], (SUB, LANES)) * locals_ref[m, pl.ds(at, SUB), :]
        mine = above + (lane8 % HALF == j).astype(F32)
        new = jnp.where(sub8 < 3, new, jnp.where(sub8 == 3, mine, 0.0))
        if isinstance(j, int):
            new = new + jnp.where((sub8 == 3) & (lane8 == joints), 1.0, 0.0)
        tree[j] = new
        state[pl.ds(at, SUB), :] = new
        diff[pl.ds(at, SUB), :] = above - new

    def descend(j, carry):
        compose(j, tree[parents[j]])
        return carry

    compose(0, (axis_lane == sub8).astype(F32))
    lax.fori_loop(1, joints, descend, 0)

    @pl.when(group == groups - 1)
    def _():
        each(0, n_src, lambda j: skin_copy(far_first(j)).start())

    for m in range(3):
        spread[m, block:LANES, :] = regressor[0:room, :]
        spread[m, extra * m : extra * (m + 1), :] = regressor[room:joints, :]
    for m in range(3):
        base = dot_nt(template[...], spread[m], EXACT)[m : m + 1, :]
        spot = iota(base.shape, 1)
        at = m * LANES
        bias[:, at : at + LANES] = jnp.where(spot >= block, base, 0.0)
        bias[:, at : at + block] = template[m : m + 1, :]
        mark = (spot >= extra * m) & (spot < extra * (m + 1))
        bias[:, 3 * LANES :] = bias[:, 3 * LANES :] + jnp.where(mark, base, 0.0)
    bias[...] = bias[...] * (group == 0).astype(F32)
    spread_parts = [jnp.concatenate(split(spread[m], 3), axis=0) for m in range(3)]

    def lay(b, at):
        for m in range(3):
            one = bas[b, m]
            sums = dot(spread_parts[m], one)
            sums = sums[0:LANES] + sums[LANES : 2 * LANES] + sums[2 * LANES :]
            wide[m * LANES : m * LANES + block, at : at + comps] = one.astype(F32)
            wide[m * LANES + block : (m + 1) * LANES, at : at + comps] = sums[block:]
            row = 3 * LANES + extra * m
            wide[row : row + extra, at : at + comps] = sums[extra * m : extra * (m + 1)]

    arrival(bas.at[1 - side], bas_r)
    for b in range(2):
        lay(b, b * LANES)
    for p, part in enumerate(split(jnp.transpose(wide[...]), PARTS)):
        table[p * 2 * LANES : (p + 1) * 2 * LANES, :] = part

    def partial(rows):
        return dot(jnp.concatenate([rows] * PARTS, axis=1), table[...]) + bias[...]

    def lead_reply():
        arrival(coeff_got.at[0], lead_r)
        rows = jnp.concatenate([coeff_got[0, 0], coeff_got[0, 1]], axis=1)
        value = partial(rows)
        lead[...] = jnp.concatenate([value[:, q * LANES : (q + 1) * LANES] for q in range(4)], axis=0)
        lead_copy.start()

    per = SUB // own

    def batch(part):
        start = part * half
        skip = 1 - part
        arrival(coeff_got.at[pl.ds(start + skip, half - skip)], coeff_r.at[part])

        def source(i, b):
            if isinstance(i, int) and i == 0 and part == 0:
                return jnp.zeros((own, LANES), F32)
            return coeff_got[start + i, b].astype(F32)

        def gather(step):
            at = step * SUB if isinstance(step, int) else pl.multiple_of(step * SUB, SUB)
            for b in range(2):
                rows = [source(step * per + i, b) for i in range(per)]
                coeff_rows[pl.ds(at, SUB), b * LANES : (b + 1) * LANES] = jnp.concatenate(rows, axis=0)

        gather(0)
        each(1, half // per, gather)
        rows = coeff_rows[...].astype(BF16)
        value = partial(rows)
        for q in range(4):
            product[q] = value[:, q * LANES : (q + 1) * LANES]
        for q in range(4):
            for c in range(own):
                sent[part, pl.ds(q * own + c, half, stride=SUB), :] = product[q, pl.ds(c, half, stride=own), :]

        @pl.when((part == 1) & (upper == 0))
        def _():
            sent_copy(start + half - 1).start()

        each(1, half, lambda j: sent_copy(start + far_in(j, part)).start())

        @pl.when((part == 1) & (upper == 1))
        def _():
            sent_copy(start + half - 1).start()

    def far_in(j, part):
        ahead = j - part
        behind = half - j - part
        return ahead + (1 - upper) * (behind - ahead)

    @pl.when(upper == 1)
    def _():
        lead_reply()

    batch(1)
    batch(0)

    @pl.when(upper == 0)
    def _():
        lead_reply()

    def flipped(ref, m, n):
        value = ref[pl.ds(m, HALF, stride=SUB), :]
        return jnp.transpose(jnp.concatenate([value, value], axis=0))[0:n]

    gains = [flipped(diff, m, SUB) for m in range(3)]
    gains = [jnp.where(lane8 < HALF, gain, 0.0) for gain in gains]
    factors = jnp.concatenate(
        [flipped(state, m, SUB)[:, 0:HALF] for m in range(3)] + [flipped(state, 3, HALF)[:, 0:HALF]], axis=0
    )
    moves = jnp.concatenate([shift[...]] * (SUB // own), axis=0)
    m_axis = jnp.minimum(iota(moves.shape, 0) // own, 2)
    moves = jnp.sum(jnp.where(iota(moves.shape, 1) == m_axis, moves, 0.0), axis=1, keepdims=True)
    moves = jnp.where(lane8 == joints, moves, 0.0)

    arrival(skin_got, skin_r)
    joint_row = iota((HALF, block), 0).astype(F32)
    for i in range(n_vert):
        grid = jnp.zeros((HALF, block), F32)
        for slot in range(slots):
            grid = jnp.where(skin_got[i, 0, slot : slot + 1, :] == joint_row, skin_got[i, 1, slot : slot + 1, :], grid)
        weights[:, i * block : (i + 1) * block] = grid
    blended = dot(factors, weights[...], EXACT)
    turns = [blended[m * SUB : (m + 1) * SUB] for m in range(3)]
    above_hi = blended[3 * SUB :].astype(BF16)
    above_lo = (blended[3 * SUB :] - above_hi.astype(F32)).astype(BF16)
    above_all = jnp.concatenate([above_hi, above_lo, above_hi], axis=0)

    packed = [jnp.where(lane8 >= block, pltpu.roll(gain, block, 1), 0.0) for gain in gains]
    rest = jnp.zeros((SUB, LANES), F32)
    for m in range(3):
        mark = (lane8 >= extra * m) & (lane8 < extra * (m + 1))
        rest = jnp.where(mark, pltpu.roll(gains[m], (extra * m - room) % LANES, 1), rest)
    packed.append(rest)
    moves = moves + pltpu.roll(moves, HALF, 1)

    def rows_of(value, number):
        count = SUB // own
        spun = [value] + [pltpu.roll(value, own * q, 0) for q in range(1, count)]
        result = []
        for m in range(number):
            one = spun[(-m) % count]
            for q in range(1, count):
                one = jnp.where(sub8 // own == q, spun[(q - m) % count], one)
            result.append(one)
        return result

    bas_copy.wait_send()

    @pl.when(first)
    def _():
        pass_copy.wait_send()

    @pl.when(jnp.logical_not(first))
    def _():
        departure(coeff_got, coeff_s)

    @pl.when(is_hub)
    def _():
        departure(coeff_got.at[pl.ds(1, n_src - 1)], relay_s.at[0])
        departure(coeff_got, relay_s.at[1])

    @pl.when(group == groups - 1)
    def _():
        for q in range(groups):
            departure(skin_got, skin_s.at[q])

    departure(sent, sent_s)
    arrival(got, sent_r)
    tiles = []
    for i in range(n_vert):
        at = i * groups * SUB
        value = got[at : at + SUB, :]
        for q in range(1, groups):
            value = value + got[at + q * SUB : at + (q + 1) * SUB, :]
        tiles.append(value)
    summed = list(tiles)
    while len(summed) > 1:
        summed = [a + b for a, b in zip(summed[0::2], summed[1::2])] + summed[len(summed) // 2 * 2 :]
    term = jnp.zeros((SUB, LANES), F32)
    for gain, spots in zip(packed, rows_of(summed[0], 4)):
        term = term + gain * spots
    half_lane = lane8 % HALF
    spread_out = moves
    for at in (0, HALF):
        near = pltpu.roll(term, (room + at) % LANES, 1)
        far = jnp.zeros((SUB, LANES), F32)
        for m in range(3):
            far = far + pltpu.roll(term, (room + at - extra * m) % LANES, 1)
        here = (lane8 >= at) & (lane8 < at + HALF)
        spread_out = spread_out + jnp.where(here & (half_lane < room), near, 0.0)
        spread_out = spread_out + jnp.where(here & (half_lane >= room) & (half_lane < joints), far, 0.0)
    term_hi = spread_out.astype(BF16)
    term_lo = (spread_out - term_hi.astype(F32)).astype(BF16)
    moved = dot(jnp.concatenate([term_hi, term_lo[:, 0:HALF]], axis=1), above_all)

    n_cols = -(-n_vert * block // LANES)
    columns = [None] * n_cols

    def put(q, value):
        columns[q] = value if columns[q] is None else columns[q] + value

    for i in range(n_vert):
        q, r = divmod(i * block, LANES)
        value = tiles[i].astype(BF16).astype(F32)
        if r:
            value = pltpu.roll(value, r, 1)
        put(q, jnp.where((lane8 >= r) & (lane8 < r + block), value, 0.0))
        if r + block > LANES:
            put(q + 1, jnp.where(lane8 < r + block - LANES, value, 0.0))
    width = n_vert * block
    for q in range(n_cols):
        at = slice(q * LANES, (q + 1) * LANES)
        value = moved[:, at]
        for m, shaped in enumerate(rows_of(columns[q], 3)):
            value = value + turns[m][:, at] * shaped
        value = value.astype(out_ref.dtype)
        size = min(LANES, width - q * LANES)
        for a in range(3):
            out_ref[a, :, q * LANES : q * LANES + size] = value[own * a : own * (a + 1), 0:size]


def body(n_vert, n_col, coeffs, shape_basis, template, regressor, quaternions, translation, parents, skin_index, skin_raw):
    own, total = coeffs.shape
    comps, _, block = shape_basis.shape
    joints = regressor.shape[0]
    slots = skin_index.shape[1]
    n_src = n_vert * (n_col // 2)
    anywhere = pl.BlockSpec(memory_space=pl.ANY)
    dma = pltpu.SemaphoreType.DMA
    out = pl.pallas_call(
        functools.partial(kernel, n_vert, n_col),
        out_shape=pltpu.VMEM((3, own, n_vert * block), BF16),
        in_specs=[anywhere] * 9,
        out_specs=pl.BlockSpec(memory_space=pltpu.VMEM),
        scratch_shapes=[
            pltpu.SMEM((joints,), jnp.int32),
            pltpu.VMEM((own, total), BF16),
            pltpu.VMEM((2, 3, block, comps), BF16),
            pltpu.VMEM((3, block), F32),
            pltpu.VMEM((joints, block), F32),
            pltpu.VMEM((own, 4, joints), F32),
            pltpu.VMEM((own, 3), F32),
            pltpu.VMEM((slots, block), jnp.int32),
            pltpu.VMEM((slots, block), F32),
            pltpu.VMEM((SUB, LANES), F32),
            pltpu.VMEM((n_col, own, LANES), BF16),
            pltpu.VMEM((n_src, 2, own, LANES), BF16),
            pltpu.VMEM((2, n_col, own, LANES), BF16),
            pltpu.VMEM((n_src * own // 2, 2 * LANES), F32),
            pltpu.VMEM((2, slots, block), F32),
            pltpu.VMEM((n_vert, 2, slots, block), F32),
            pltpu.VMEM((3, LANES, block), F32),
            pltpu.VMEM((4 * LANES, 2 * LANES), F32),
            pltpu.VMEM((PARTS * 2 * LANES, 4 * LANES), BF16),
            pltpu.VMEM((1, 4 * LANES), F32),
            pltpu.VMEM((4, n_src * own // 2, LANES), F32),
            pltpu.VMEM((SUB, LANES), F32),
            pltpu.VMEM((2, n_src // 2 * SUB, LANES), F32),
            pltpu.VMEM((n_src * SUB, LANES), F32),
            pltpu.VMEM((joints, SUB, LANES), F32),
            pltpu.VMEM((HALF * SUB, LANES), F32),
            pltpu.VMEM((HALF * SUB, LANES), F32),
            pltpu.VMEM((3, HALF * SUB, LANES), F32),
            pltpu.VMEM((HALF, -(-n_vert * block // LANES) * LANES), F32),
            dma((9,)),
            dma,
            dma,
            dma,
            dma((2,)),
            dma,
            dma,
            dma((2,)),
            dma((2,)),
            dma((n_col // 2,)),
            dma,
            dma,
            dma,
        ],
        compiler_params=pltpu.CompilerParams(collective_id=0, has_side_effects=True),
    )(
        parents,
        coeffs,
        jnp.transpose(shape_basis, (1, 2, 0)),
        template,
        regressor,
        quaternions,
        translation,
        jnp.transpose(skin_index),
        jnp.transpose(skin_raw),
    )
    return jnp.transpose(out, (1, 0, 2))


def solution(mesh):
    in_specs = (
        P(("vert", "col"), None),
        P("col", None, "vert"),
        P(None, "vert"),
        P(None, "vert"),
        P(("vert", "col"), None, None),
        P(("vert", "col"), None),
        P(),
        P("vert", None),
        P("vert", None),
    )
    out_specs = P(("vert", "col"), None, None)
    step = functools.partial(body, mesh.shape["vert"], mesh.shape["col"])
    return jax.shard_map(step, mesh=mesh, in_specs=in_specs, out_specs=out_specs, check_vma=False)
```

```python
import functools

import jax
import jax.numpy as jnp
from jax import lax
from jax.experimental import pallas as pl
from jax.experimental.pallas import tpu as pltpu
from jax.sharding import PartitionSpec as P

MESH = pl.DeviceIdType.MESH
LANES = 128
HALF = 64
SUB = 8
PARTS = 2
F32 = jnp.float32
BF16 = jnp.bfloat16
EXACT = lax.Precision.HIGHEST


def iota(shape, dim):
    return lax.broadcasted_iota(jnp.int32, shape, dim)


def dot(a, b, precision=None):
    return jnp.dot(a, b, precision=precision, preferred_element_type=F32)


def dot_nt(a, b, precision=None):
    return lax.dot_general(a, b, (((1,), (1,)), ((), ())), precision=precision, preferred_element_type=F32)


def each(first, count, step):
    if count - first <= 16:
        for k in range(first, count):
            step(k)
    else:

        def one(k, carry):
            step(k)
            return carry

        lax.fori_loop(first, count, one, 0)


def split(value, count):
    parts = []
    for _ in range(count):
        part = value.astype(BF16)
        value = value - part.astype(F32)
        parts.append(part)
    return parts


def kernel(
    n_vert,
    n_col,
    parents_hbm,
    coeffs_hbm,
    basis_hbm,
    template_hbm,
    regressor_hbm,
    quat_hbm,
    shift_hbm,
    index_hbm,
    raw_hbm,
    out_ref,
    parents,
    coeff_in,
    bas,
    template,
    regressor,
    quat,
    shift,
    index_in,
    raw_in,
    quat_rows,
    coeff_out,
    coeff_got,
    lead_got,
    passed,
    coeff_rows,
    skin_out,
    skin_got,
    spread,
    wide,
    table,
    bias,
    product,
    lead,
    sent,
    got,
    tree,
    state,
    diff,
    locals_ref,
    factors,
    weights,
    above,
    local_s,
    bas_s,
    bas_r,
    coeff_s,
    coeff_r,
    lead_s,
    lead_r,
    passed_s,
    passed_r,
    relay_s,
    skin_s,
    skin_r,
    sent_s,
    sent_r,
):
    me = lax.axis_index("vert")
    col = lax.axis_index("col")
    own, total = coeffs_hbm.shape
    _, block, comps = basis_hbm.shape
    joints = regressor_hbm.shape[0]
    slots = index_hbm.shape[0]
    groups = n_col // 2
    n_src = n_vert * groups
    room = LANES - block
    extra = joints - room

    group = col // 2
    side = col % 2
    mine = me * groups + group
    first = mine == 0
    hub = n_vert // 2
    is_hub = (me == hub) & (col == 1)
    partner = (me, 2 * group + 1 - side)
    upper = me // hub

    def place(i, parity):
        return (i // groups, 2 * (i % groups) + parity)

    def across(i):
        return place(i, 1 - side)

    def far_first(j):
        return j + (1 - upper) * (n_src - 1 - 2 * j)

    barrier = pltpu.get_barrier_semaphore()

    def hello(target):
        pl.semaphore_signal(barrier, inc=1, device_id=target, device_id_type=MESH)

    @pl.when(is_hub)
    def _():
        hello((0, 1))

    @pl.when(is_hub | first)
    def _():
        hello(across(0))

    @pl.when((side == 1) & jnp.logical_not(is_hub))
    def _():
        hello((hub, 1))

    each(1, n_src, lambda j: hello(across(j)))

    pairs = [
        (coeffs_hbm, coeff_in),
        (basis_hbm, bas.at[side]),
        (index_hbm, index_in),
        (raw_hbm, raw_in),
        (parents_hbm, parents),
        (quat_hbm, quat),
        (shift_hbm, shift),
        (template_hbm, template),
        (regressor_hbm, regressor),
    ]
    loads = [pltpu.make_async_copy(src, dst, local_s.at[i]) for i, (src, dst) in enumerate(pairs)]
    for load in loads:
        load.start()

    sub8 = iota((SUB, LANES), 0)
    lane8 = iota((SUB, LANES), 1)
    axis_lane = jnp.minimum((lane8 % SUB) // own, 2)
    quat_rows[...] = jnp.zeros(quat_rows.shape, F32)
    weights[...] = jnp.zeros(weights.shape, F32)
    factors[...] = jnp.zeros(factors.shape, F32)
    tree[...] = jnp.zeros(tree.shape, F32)
    state[...] = jnp.zeros(state.shape, F32)
    diff[...] = jnp.zeros(diff.shape, F32)
    coeff_out[...] = jnp.zeros(coeff_out.shape, BF16)
    spread[...] = jnp.zeros(spread.shape, F32)
    wide[...] = jnp.zeros(wide.shape, F32)
    bias[...] = jnp.zeros(bias.shape, F32)
    for load in loads:
        load.wait()

    mine_coeffs = coeff_in[...].astype(F32)
    for kb in range(n_col):
        coeff_out[kb, :, 0:comps] = mine_coeffs[:, kb * comps : (kb + 1) * comps].astype(BF16)
    raw = raw_in[...]
    skin_out[0] = index_in[...].astype(F32)
    skin_out[1] = raw / jnp.sum(raw, axis=0, keepdims=True)

    def remote(src, dst, send, recv, target):
        return pltpu.make_async_remote_copy(
            src_ref=src, dst_ref=dst, send_sem=send, recv_sem=recv, device_id=target, device_id_type=MESH
        )

    bas_copy = remote(bas.at[side], bas.at[side], bas_s, bas_r, partner)

    def two(i):
        return pl.ds(2 * (i % groups), 2)

    half = n_src // 2

    def coeff_sem(i):
        return coeff_r.at[i // half]

    def coeff_copy(i):
        return remote(coeff_out.at[two(i)], coeff_got.at[mine], coeff_s, coeff_sem(mine), across(i))

    def arrival(ref, recv):
        remote(ref, ref, bas_s, recv, partner).wait_recv()

    def departure(ref, send):
        remote(ref, ref, send, bas_r, partner).wait_send()

    pass_copy = remote(coeff_out, passed.at[side], passed_s, passed_r.at[side], (hub, 1))

    def relay_copy(k, i):
        return remote(passed.at[k, two(i)], lead_got.at[k], relay_s.at[k], lead_r.at[k], place(i, 1))

    def skin_copy(i):
        return remote(skin_out, skin_got.at[me], skin_s.at[i // n_vert], skin_r, across(i))

    def tile(ref, i):
        start = i * SUB if isinstance(i, int) else pl.multiple_of(i * SUB, SUB)
        return ref.at[pl.ds(start, SUB)]

    def sent_copy(i):
        return remote(tile(sent.at[i // half], i % half), tile(got, mine), sent_s, sent_r, across(i))

    def lead_copy(k):
        return remote(lead.at[k], tile(got, mine), sent_s if k == 0 else lead_s, sent_r, (0, k))

    hub_index = hub * groups
    expected = n_src + is_hub.astype(jnp.int32) * (n_src - 1)
    pl.semaphore_wait(barrier, jnp.where(first, 2, expected))
    bas_copy.start()

    @pl.when(first)
    def _():
        pass_copy.start()

    @pl.when(is_hub)
    def _():
        arrival(passed.at[0], passed_r.at[0])
        each(0, half // 2, lambda j: relay_copy(0, n_src - 1 - j).start())
        arrival(passed.at[1], passed_r.at[1])
        each(0, half // 2, lambda j: relay_copy(1, n_src - 1 - j).start())
        for k in range(2):
            each(half // 2, n_src - 1 - hub_index, lambda j: relay_copy(k, n_src - 1 - j).start())
            pltpu.make_async_copy(passed.at[k, two(hub_index)], lead_got.at[k], lead_r.at[k]).start()
            each(0, hub_index, lambda i: relay_copy(k, i).start())

    @pl.when(jnp.logical_not(first))
    def _():
        each(0, n_src, lambda j: coeff_copy(far_first(j)).start())

    for c in range(own):
        quat_rows[4 * c : 4 * c + 4, 0:joints] = quat[c]
    q_row = iota((LANES, SUB), 0)
    q_col = iota((LANES, SUB), 1)
    w, x, y, z = [
        jnp.transpose(dot((q_col == (q_row % own) * 4 + comp).astype(F32), quat_rows[...], EXACT))[0:HALF] for comp in range(4)
    ]
    s = 2.0 / (w * w + x * x + y * y + z * z)
    matrix = [
        [1.0 - s * (y * y + z * z), s * (x * y - w * z), s * (x * z + w * y)],
        [s * (x * y + w * z), 1.0 - s * (x * x + z * z), s * (y * z - w * x)],
        [s * (x * z - w * y), s * (y * z + w * x), 1.0 - s * (x * x + y * y)],
    ]
    for m in range(3):
        for b in range(3):
            locals_ref[m, pl.ds(b, HALF, stride=SUB), :] = matrix[m][b]

    def compose(j, above):
        at = pl.multiple_of(j * SUB, SUB)
        new = jnp.zeros((SUB, LANES), F32)
        for m in range(3):
            new = new + jnp.broadcast_to(above[m : m + 1, :], (SUB, LANES)) * locals_ref[m, pl.ds(at, SUB), :]
        mine = above + (lane8 % HALF == j).astype(F32)
        new = jnp.where(sub8 < 3, new, jnp.where(sub8 == 3, mine, 0.0))
        if isinstance(j, int):
            new = new + jnp.where((sub8 == 3) & (lane8 == joints), 1.0, 0.0)
        tree[j] = new
        state[pl.ds(at, SUB), :] = new
        diff[pl.ds(at, SUB), :] = above - new

    def descend(j, carry):
        compose(j, tree[parents[j]])
        return carry

    compose(0, (axis_lane == sub8).astype(F32))
    lax.fori_loop(1, joints, descend, 0)

    @pl.when(group == groups - 1)
    def _():
        each(0, n_src, lambda j: skin_copy(far_first(j)).start())

    for m in range(3):
        spread[m, block:LANES, :] = regressor[0:room, :]
        spread[m, extra * m : extra * (m + 1), :] = regressor[room:joints, :]
    for m in range(3):
        base = dot_nt(template[...], spread[m], EXACT)[m : m + 1, :]
        spot = iota(base.shape, 1)
        at = m * LANES
        bias[:, at : at + LANES] = jnp.where(spot >= block, base, 0.0)
        bias[:, at : at + block] = template[m : m + 1, :]
        mark = (spot >= extra * m) & (spot < extra * (m + 1))
        bias[:, 3 * LANES :] = bias[:, 3 * LANES :] + jnp.where(mark, base, 0.0)
    bias[...] = bias[...] * (group == 0).astype(F32)
    spread_parts = [jnp.concatenate(split(spread[m], 3), axis=0) for m in range(3)]

    def lay(b, at):
        for m in range(3):
            one = bas[b, m]
            sums = dot(spread_parts[m], one)
            sums = sums[0:LANES] + sums[LANES : 2 * LANES] + sums[2 * LANES :]
            wide[m * LANES : m * LANES + block, at : at + comps] = one.astype(F32)
            wide[m * LANES + block : (m + 1) * LANES, at : at + comps] = sums[block:]
            row = 3 * LANES + extra * m
            wide[row : row + extra, at : at + comps] = sums[extra * m : extra * (m + 1)]

    arrival(bas.at[1 - side], bas_r)
    for b in range(2):
        lay(b, b * LANES)
    for p, part in enumerate(split(jnp.transpose(wide[...]), PARTS)):
        table[p * 2 * LANES : (p + 1) * 2 * LANES, :] = part

    def partial(rows):
        return dot(jnp.concatenate([rows] * PARTS, axis=1), table[...]) + bias[...]

    def lead_reply():
        rows = []
        for k in range(2):
            arrival(lead_got.at[k], lead_r.at[k])
        for k in range(2):
            rows.append(jnp.concatenate([lead_got[k, 0], lead_got[k, 1]], axis=1).astype(F32))
        value = partial(jnp.concatenate(rows, axis=0).astype(BF16))
        for k in range(2):
            part = value[own * k : own * (k + 1)]
            lead[k] = jnp.concatenate([part[:, q * LANES : (q + 1) * LANES] for q in range(4)], axis=0)
        lead_copy(0).start()

        @pl.when(mine > 0)
        def _():
            lead_copy(1).start()

        @pl.when(mine == 0)
        def _():
            pltpu.make_async_copy(lead.at[1], tile(got, mine), sent_r).start()

    per = SUB // own

    def batch(part):
        start = part * half
        skip = 1 - part
        arrival(coeff_got.at[pl.ds(start + skip, half - skip)], coeff_r.at[part])

        def source(i, b):
            if isinstance(i, int) and i == 0 and part == 0:
                return jnp.zeros((own, LANES), F32)
            return coeff_got[start + i, b].astype(F32)

        def gather(step):
            at = step * SUB if isinstance(step, int) else pl.multiple_of(step * SUB, SUB)
            for b in range(2):
                rows = [source(step * per + i, b) for i in range(per)]
                coeff_rows[pl.ds(at, SUB), b * LANES : (b + 1) * LANES] = jnp.concatenate(rows, axis=0)

        gather(0)
        each(1, half // per, gather)
        rows = coeff_rows[...].astype(BF16)
        value = partial(rows)
        for q in range(4):
            product[q] = value[:, q * LANES : (q + 1) * LANES]
        for q in range(4):
            for c in range(own):
                sent[part, pl.ds(q * own + c, half, stride=SUB), :] = product[q, pl.ds(c, half, stride=own), :]

        @pl.when((part == 1) & (upper == 0))
        def _():
            sent_copy(start + half - 1).start()

        each(1, half, lambda j: sent_copy(start + far_in(j, part)).start())

        @pl.when((part == 1) & (upper == 1))
        def _():
            sent_copy(start + half - 1).start()

    def far_in(j, part):
        ahead = j - part
        behind = half - j - part
        return ahead + (1 - upper) * (behind - ahead)

    @pl.when((upper == 1) & (side == 1))
    def _():
        lead_reply()

    batch(1)
    batch(0)

    @pl.when((upper == 0) & (side == 1))
    def _():
        lead_reply()

    def flipped(ref, m, n):
        value = ref[pl.ds(m, HALF, stride=SUB), :]
        return jnp.transpose(jnp.concatenate([value, value], axis=0))[0:n]

    gains = [flipped(diff, m, SUB) for m in range(3)]
    gains = [jnp.where(lane8 < HALF, gain, 0.0) for gain in gains]
    for m in range(3):
        factors[m * SUB : (m + 1) * SUB, :] = flipped(state, m, SUB)[:, 0:HALF]
    line = flipped(state, 3, HALF)[:, 0:HALF]
    factors[3 * SUB + block : 3 * SUB + LANES, :] = line[0:room]
    for m in range(3):
        factors[3 * SUB + extra * m : 3 * SUB + extra * (m + 1), :] = line[room:joints]
    spare = 3 * extra
    factors[3 * SUB + spare : 3 * SUB + spare + 1, :] = line[joints : joints + 1]
    moves = jnp.concatenate([shift[...]] * (SUB // own), axis=0)
    m_axis = jnp.minimum(iota(moves.shape, 0) // own, 2)
    moves = jnp.sum(jnp.where(iota(moves.shape, 1) == m_axis, moves, 0.0), axis=1, keepdims=True)
    moves = jnp.where(lane8 == spare, moves, 0.0)

    arrival(skin_got, skin_r)
    joint_row = iota((HALF, block), 0).astype(F32)
    for i in range(n_vert):
        grid = jnp.zeros((HALF, block), F32)
        for slot in range(slots):
            grid = jnp.where(skin_got[i, 0, slot : slot + 1, :] == joint_row, skin_got[i, 1, slot : slot + 1, :], grid)
        weights[:, i * block : (i + 1) * block] = grid
    blended = dot(factors[...], weights[...], EXACT)
    turns = [blended[m * SUB : (m + 1) * SUB] for m in range(3)]
    above_hi = blended[3 * SUB :].astype(BF16)
    above_lo = (blended[3 * SUB :] - above_hi.astype(F32)).astype(BF16)
    above[0:LANES, :] = above_hi
    above[LANES : 2 * LANES, :] = above_hi
    above[2 * LANES :, :] = above_lo

    packed = [jnp.where(lane8 >= block, pltpu.roll(gain, block, 1), 0.0) for gain in gains]
    rest = jnp.zeros((SUB, LANES), F32)
    for m in range(3):
        mark = (lane8 >= extra * m) & (lane8 < extra * (m + 1))
        rest = jnp.where(mark, pltpu.roll(gains[m], (extra * m - room) % LANES, 1), rest)
    packed.append(rest)

    def rows_of(value, number):
        count = SUB // own
        spun = [value] + [pltpu.roll(value, own * q, 0) for q in range(1, count)]
        result = []
        for m in range(number):
            one = spun[(-m) % count]
            for q in range(1, count):
                one = jnp.where(sub8 // own == q, spun[(q - m) % count], one)
            result.append(one)
        return result

    bas_copy.wait_send()

    @pl.when(first)
    def _():
        pass_copy.wait_send()

    @pl.when(jnp.logical_not(first))
    def _():
        departure(coeff_got, coeff_s)

    @pl.when(is_hub)
    def _():
        for k in range(2):
            departure(coeff_got.at[pl.ds(1, n_src - 1)], relay_s.at[k])

    @pl.when(group == groups - 1)
    def _():
        for q in range(groups):
            departure(skin_got, skin_s.at[q])

    @pl.when(side == 1)
    def _():
        departure(got, sent_s)

    @pl.when(side == 0)
    def _():
        departure(got.at[pl.ds(SUB, (n_src - 1) * SUB)], sent_s)

    @pl.when((side == 1) & (mine > 0))
    def _():
        departure(lead.at[1], lead_s)
    arrival(got, sent_r)
    tiles = []
    for i in range(n_vert):
        at = i * groups * SUB
        value = got[at : at + SUB, :]
        for q in range(1, groups):
            value = value + got[at + q * SUB : at + (q + 1) * SUB, :]
        tiles.append(value)
    summed = list(tiles)
    while len(summed) > 1:
        summed = [a + b for a, b in zip(summed[0::2], summed[1::2])] + summed[len(summed) // 2 * 2 :]
    term = moves
    for gain, spots in zip(packed, rows_of(summed[0], 4)):
        term = term + gain * spots
    term_hi = term.astype(BF16)
    term_lo = (term - term_hi.astype(F32)).astype(BF16)
    moved = dot(jnp.concatenate([term_hi, term_lo], axis=1), above[0 : 2 * LANES, :]) + dot(term_hi, above[2 * LANES :, :])

    n_cols = -(-n_vert * block // LANES)
    columns = [None] * n_cols

    def put(q, value):
        columns[q] = value if columns[q] is None else columns[q] + value

    for i in range(n_vert):
        q, r = divmod(i * block, LANES)
        value = tiles[i].astype(BF16).astype(F32)
        if r:
            value = pltpu.roll(value, r, 1)
        put(q, jnp.where((lane8 >= r) & (lane8 < r + block), value, 0.0))
        if r + block > LANES:
            put(q + 1, jnp.where(lane8 < r + block - LANES, value, 0.0))
    width = n_vert * block
    for q in range(n_cols):
        at = slice(q * LANES, (q + 1) * LANES)
        value = moved[:, at]
        for m, shaped in enumerate(rows_of(columns[q], 3)):
            value = value + turns[m][:, at] * shaped
        value = value.astype(out_ref.dtype)
        size = min(LANES, width - q * LANES)
        for a in range(3):
            out_ref[a, :, q * LANES : q * LANES + size] = value[own * a : own * (a + 1), 0:size]


def body(n_vert, n_col, coeffs, shape_basis, template, regressor, quaternions, translation, parents, skin_index, skin_raw):
    own, total = coeffs.shape
    comps, _, block = shape_basis.shape
    joints = regressor.shape[0]
    slots = skin_index.shape[1]
    n_src = n_vert * (n_col // 2)
    anywhere = pl.BlockSpec(memory_space=pl.ANY)
    dma = pltpu.SemaphoreType.DMA
    out = pl.pallas_call(
        functools.partial(kernel, n_vert, n_col),
        out_shape=pltpu.VMEM((3, own, n_vert * block), BF16),
        in_specs=[anywhere] * 9,
        out_specs=pl.BlockSpec(memory_space=pltpu.VMEM),
        scratch_shapes=[
            pltpu.SMEM((joints,), jnp.int32),
            pltpu.VMEM((own, total), BF16),
            pltpu.VMEM((2, 3, block, comps), BF16),
            pltpu.VMEM((3, block), F32),
            pltpu.VMEM((joints, block), F32),
            pltpu.VMEM((own, 4, joints), F32),
            pltpu.VMEM((own, 3), F32),
            pltpu.VMEM((slots, block), jnp.int32),
            pltpu.VMEM((slots, block), F32),
            pltpu.VMEM((SUB, LANES), F32),
            pltpu.VMEM((n_col, own, LANES), BF16),
            pltpu.VMEM((n_src, 2, own, LANES), BF16),
            pltpu.VMEM((2, 2, own, LANES), BF16),
            pltpu.VMEM((2, n_col, own, LANES), BF16),
            pltpu.VMEM((n_src * own // 2, 2 * LANES), F32),
            pltpu.VMEM((2, slots, block), F32),
            pltpu.VMEM((n_vert, 2, slots, block), F32),
            pltpu.VMEM((3, LANES, block), F32),
            pltpu.VMEM((4 * LANES, 2 * LANES), F32),
            pltpu.VMEM((PARTS * 2 * LANES, 4 * LANES), BF16),
            pltpu.VMEM((1, 4 * LANES), F32),
            pltpu.VMEM((4, n_src * own // 2, LANES), F32),
            pltpu.VMEM((2, SUB, LANES), F32),
            pltpu.VMEM((2, n_src // 2 * SUB, LANES), F32),
            pltpu.VMEM((n_src * SUB, LANES), F32),
            pltpu.VMEM((joints, SUB, LANES), F32),
            pltpu.VMEM((HALF * SUB, LANES), F32),
            pltpu.VMEM((HALF * SUB, LANES), F32),
            pltpu.VMEM((3, HALF * SUB, LANES), F32),
            pltpu.VMEM((3 * SUB + LANES, HALF), F32),
            pltpu.VMEM((HALF, -(-n_vert * block // LANES) * LANES), F32),
            pltpu.VMEM((3 * LANES, -(-n_vert * block // LANES) * LANES), BF16),
            dma((9,)),
            dma,
            dma,
            dma,
            dma((2,)),
            dma,
            dma((2,)),
            dma,
            dma((2,)),
            dma((2,)),
            dma((n_col // 2,)),
            dma,
            dma,
            dma,
        ],
        compiler_params=pltpu.CompilerParams(collective_id=0, has_side_effects=True),
    )(
        parents,
        coeffs,
        jnp.transpose(shape_basis, (1, 2, 0)),
        template,
        regressor,
        quaternions,
        translation,
        jnp.transpose(skin_index),
        jnp.transpose(skin_raw),
    )
    return jnp.transpose(out, (1, 0, 2))


def solution(mesh):
    in_specs = (
        P(("vert", "col"), None),
        P("col", None, "vert"),
        P(None, "vert"),
        P(None, "vert"),
        P(("vert", "col"), None, None),
        P(("vert", "col"), None),
        P(),
        P("vert", None),
        P("vert", None),
    )
    out_specs = P(("vert", "col"), None, None)
    step = functools.partial(body, mesh.shape["vert"], mesh.shape["col"])
    return jax.shard_map(step, mesh=mesh, in_specs=in_specs, out_specs=out_specs, check_vma=False)
```
